32 devices in a mesh: blk: 8 (over y, x, core), grp: 4 (over z).
Axes of the slice: x: 2, y: 2, z: 4, core: 2. Of those that a mesh axis runs over, the one named last changes fastest.
Arguments:
- trial_vec: float32 [1536, 24], P(('blk', 'grp')), may hold values from -6 to 6
- resid_vec: float32 [1536, 24], P(('blk', 'grp')), may hold values from -6 to 6
- search_dir: float32 [1536, 24], P(('blk', 'grp')), may hold values from -6 to 6
- trial_img: float32 [1536, 24], P(('blk', 'grp')), may hold values from -12 to 12
- search_img: float32 [1536, 24], P(('blk', 'grp')), may hold values from -12 to 12
- dens_exch: bfloat16 [1536, 20480], P(('blk', 'grp')), may hold values from -0.15625 to 0.15625
- dens_direct: bfloat16 [1536, 20480], P(('blk', 'grp')), may hold values from -0.15625 to 0.15625
- screen_mat: bfloat16 [20480, 20480], P('grp', 'blk'), may hold values from -0.0390625 to 0.0390625
- coulomb: float32 [20480], replicated, may hold values from 0.2 to 2
- valence_energy: float32 [96], replicated, may hold values from -3 to -1
- conduct_energy: float32 [256], replicated, may hold values from 0.5 to 3
- valence_index: int32 [1536], P(('blk', 'grp')), may hold values from 0 to 95, as said below
- conduct_index: int32 [1536], P(('blk', 'grp')), may hold values from 0 to 255, as said below
- ritz_coef: float32 [72, 24], replicated, may hold values from -1.75 to 1.75
Outputs:
- next_trial: float32 [1536, 24], P(('blk', 'grp'))
- next_trial_img: float32 [1536, 24], P(('blk', 'grp'))
- next_search: float32 [1536, 24], P(('blk', 'grp'))
- next_search_img: float32 [1536, 24], P(('blk', 'grp'))
- gram_matrix: float32 [72, 72], replicated
The draws below stay inside these ranges and needn't reach their ends.
Inputs may be any that keep to these rules, and one draw needn't show every extreme that they name: `valence_index`: no two pairs have both the same valence band and the same conduction band. `conduct_index`: no two pairs have both the same valence band and the same conduction band.
All inputs are finite; a program needn't handle non-finite values.
Results may differ from the reference program's by a relative error of at most 0.0034.
Values may be sent and summed in bfloat16 or wider, within the bound.
No kernel may reach another device: no remote copies, remote signals or barrier semaphores. Data moves between devices by JAX's collectives and lax.ppermute only.
A program may use at most 64 MiB of HBM per device.

```python
import math
import jax
import jax.numpy as jnp
from jax import lax

NG = 20480
NE = 24
NV = 96
NC = 256
PAIRS = 1536


def pair_numbers(key):
    mixed = jax.random.permutation(jax.random.fold_in(key, 7), NV * NC)
    return mixed[:PAIRS].astype(jnp.int32)


def draw_valence_index(key, part):
    return (pair_numbers(key) // NC).astype(jnp.int32)


def draw_conduct_index(key, part):
    return (pair_numbers(key) % NC).astype(jnp.int32)


def level_of(own_key, extent, cuts, low, top_value):
    gain = 1.0
    for position, blocks in cuts:
        draws = jax.random.uniform(jax.random.fold_in(jax.random.fold_in(own_key, 6), position), (blocks,), jnp.float32, low / len(cuts), top_value / len(cuts))
        gain = gain * jnp.repeat(jnp.exp(draws), extent[position] // blocks).reshape((-1,) + (1,) * (len(extent) - 1 - position))
    return gain


def bell_draw(key, dims, width, bound, cuts=(), kind=jnp.bfloat16):
    entries = width * jax.random.normal(key, dims, jnp.float32)
    if cuts:
        entries = entries * level_of(key, dims, cuts, -0.22, 0.18)
    return jnp.clip(entries, -bound, bound).astype(kind)


def setup_inputs(seed: int = 0) -> dict:
    keys = jax.random.split(jax.random.key(seed), 15)
    return {
        "trial_vec": bell_draw(keys[0], (PAIRS, NE), 1.0, 6.0, ((0, 32),), jnp.float32),
        "resid_vec": bell_draw(keys[1], (PAIRS, NE), 1.0, 6.0, ((0, 32),), jnp.float32),
        "search_dir": bell_draw(keys[2], (PAIRS, NE), 1.0, 6.0, ((0, 32),), jnp.float32),
        "trial_img": bell_draw(keys[3], (PAIRS, NE), 2.0, 12.0, ((0, 32),), jnp.float32),
        "search_img": bell_draw(keys[4], (PAIRS, NE), 2.0, 12.0, ((0, 32),), jnp.float32),
        "dens_exch": bell_draw(keys[5], (PAIRS, NG), PAIRS ** -0.5, 0.15625, ((0, 32),)),
        "dens_direct": bell_draw(keys[6], (PAIRS, NG), PAIRS ** -0.5, 0.15625, ((0, 32),)),
        "screen_mat": bell_draw(keys[7], (NG, NG), NG ** -0.5, 0.0390625, ((0, 4), (1, 8))),
        "coulomb": jnp.clip(jnp.exp(jax.random.uniform(keys[8], (NG,), jnp.float32, math.log(0.2), math.log(2.0))), 0.2, 2.0),
        "valence_energy": jnp.clip(jax.random.uniform(keys[9], (NV,), jnp.float32, -3.0, -1.0), -3.0, -1.0),
        "conduct_energy": jnp.clip(jax.random.uniform(keys[10], (NC,), jnp.float32, 0.5, 3.0), 0.5, 3.0),
        "valence_index": draw_valence_index(jax.random.fold_in(keys[14], 71), 0),
        "conduct_index": draw_conduct_index(jax.random.fold_in(keys[14], 71), 0),
        "ritz_coef": bell_draw(keys[13], (3 * NE, NE), 0.3, 1.75, (), jnp.float32),
    }


def tdot(left, right):
    return jnp.dot(left, right, precision=lax.Precision.HIGHEST)


def reference(trial_vec, resid_vec, search_dir, trial_img, search_img, dens_exch, dens_direct, screen_mat, coulomb, valence_energy, conduct_energy, valence_index, conduct_index, ritz_coef):
    gap = conduct_energy[conduct_index.astype(jnp.int32)] - valence_energy[valence_index.astype(jnp.int32)]
    resid_half = resid_vec.astype(jnp.bfloat16)
    proj = jnp.dot(dens_exch.T, resid_half, preferred_element_type=jnp.float32)
    weighted = (coulomb[:, None] * proj).astype(jnp.bfloat16)
    exch_term = jnp.dot(dens_exch, weighted, preferred_element_type=jnp.float32)
    seen = jnp.dot(dens_direct.T, resid_half, preferred_element_type=jnp.float32).astype(jnp.bfloat16)
    screened = jnp.dot(screen_mat, seen, preferred_element_type=jnp.float32).astype(jnp.bfloat16)
    direct_term = jnp.dot(dens_direct, screened, preferred_element_type=jnp.float32)
    resid_img = gap[:, None] * resid_vec + 2.0 * exch_term - direct_term
    basis = jnp.concatenate([trial_vec, resid_vec, search_dir], axis=1)
    images = jnp.concatenate([trial_img, resid_img, search_img], axis=1)
    gram_matrix = tdot(basis.T, images)
    lower = ritz_coef[NE:]
    next_trial = tdot(basis, ritz_coef)
    next_trial_img = tdot(images, ritz_coef)
    next_search = tdot(jnp.concatenate([resid_vec, search_dir], axis=1), lower)
    next_search_img = tdot(jnp.concatenate([resid_img, search_img], axis=1), lower)
    return next_trial, next_trial_img, next_search, next_search_img, gram_matrix
```

```python
import jax
import jax.numpy as jnp
from jax import lax
from jax.experimental import pallas as pl
from jax.experimental.pallas import tpu as pltpu
from jax.sharding import PartitionSpec as P


F32 = jnp.float32
HALF = jnp.bfloat16
ACROSS_ROWS = (((0,), (0,)), ((), ()))
ACROSS_LANES = (((1,), (1,)), ((), ()))


def exact_dot(left, right):
    return jnp.dot(left, right, precision=lax.Precision.HIGHEST)


def swap(value, axis, offset):
    size = lax.axis_size(axis)
    return lax.ppermute(value, axis, [(i, i ^ offset) for i in range(size)])


def project(dens, resid_half, place, blk, grp):
    pairs, total = dens.shape
    excitons = resid_half.shape[1]
    block = total // blk
    piece = block // grp

    def body(place_ref, resid_ref, kept_ref, sent_ref, keep_ref, send_ref):
        kept = lax.dot_general(resid_ref[...], kept_ref[...], ACROSS_ROWS, preferred_element_type=F32)
        sent = lax.dot_general(resid_ref[...], sent_ref[...], ACROSS_ROWS, preferred_element_type=F32)
        for z in range(grp):
            lanes = slice(z * piece, (z + 1) * piece)
            slot = z ^ place_ref[1]
            keep_ref[0, slot] = kept[:, lanes]
            send_ref[0, slot] = sent[:, lanes].astype(HALF)

    out_spec = pl.BlockSpec((1, grp, excitons, piece), lambda j, at: (j, 0, 0, 0))
    shape = (blk // 2, grp, excitons, piece)
    return pl.pallas_call(
        body,
        grid_spec=pltpu.PrefetchScalarGridSpec(
            num_scalar_prefetch=1,
            grid=(blk // 2,),
            in_specs=[
                pl.BlockSpec((pairs, excitons), lambda j, at: (0, 0)),
                pl.BlockSpec((pairs, block), lambda j, at: (0, (2 * j) ^ at[0])),
                pl.BlockSpec((pairs, block), lambda j, at: (0, (2 * j + 1) ^ at[0])),
            ],
            out_specs=[out_spec, out_spec],
        ),
        out_shape=[jax.ShapeDtypeStruct(shape, F32), jax.ShapeDtypeStruct(shape, HALF)],
    )(place, resid_half, dens, dens)


def screen(screen_mat, seen, place, blk):
    rows, cols = screen_mat.shape
    excitons = seen.shape[0]
    piece = rows // blk

    def body(place_ref, seen_ref, kept_ref, sent_ref, keep_ref, send_ref):
        keep_ref[0] = lax.dot_general(
            seen_ref[...], kept_ref[...], ACROSS_LANES, preferred_element_type=F32
        )
        send_ref[0] = lax.dot_general(
            seen_ref[...], sent_ref[...], ACROSS_LANES, preferred_element_type=F32
        ).astype(HALF)

    out_spec = pl.BlockSpec((1, excitons, piece), lambda j, at: (j, 0, 0))
    shape = (blk // 2, excitons, piece)
    return pl.pallas_call(
        body,
        grid_spec=pltpu.PrefetchScalarGridSpec(
            num_scalar_prefetch=1,
            grid=(blk // 2,),
            in_specs=[
                pl.BlockSpec((excitons, cols), lambda j, at: (0, 0)),
                pl.BlockSpec((piece, cols), lambda j, at: ((2 * j) ^ at[0], 0)),
                pl.BlockSpec((piece, cols), lambda j, at: ((2 * j + 1) ^ at[0], 0)),
            ],
            out_specs=[out_spec, out_spec],
        ),
        out_shape=[jax.ShapeDtypeStruct(shape, F32), jax.ShapeDtypeStruct(shape, HALF)],
    )(place, seen, screen_mat, screen_mat)


def expand(dens, near, far, place, blk, grp, grp_major):
    pairs, total = dens.shape
    excitons, piece = near.shape[2:]

    def body(place_ref, dens_ref, near_ref, far_ref, out_ref):
        acc = jnp.zeros((pairs, excitons), F32)
        odd = place_ref[0] & 1
        for pair in range(blk // 2):
            slot = pair ^ (place_ref[0] >> 1)
            for z in range(grp):
                deep = z ^ place_ref[1]
                own = near_ref[slot, deep]
                other = far_ref[slot, deep]
                for bit in range(2):
                    b = 2 * pair + bit
                    at = (z * blk + b) if grp_major else (b * grp + z)
                    value = jnp.where(odd == bit, own, other)
                    acc += lax.dot_general(
                        dens_ref[:, at * piece : (at + 1) * piece],
                        value,
                        ACROSS_LANES,
                        preferred_element_type=F32,
                    )
        out_ref[...] = acc

    vmem = pl.BlockSpec(memory_space=pltpu.VMEM)
    return pl.pallas_call(
        body,
        in_specs=[pl.BlockSpec(memory_space=pltpu.SMEM), vmem, vmem, vmem],
        out_specs=vmem,
        out_shape=jax.ShapeDtypeStruct((pairs, excitons), F32),
    )(place, dens, near, far)


def spread_sum(kept, sent):
    pairs = kept.shape[0]
    part = kept + swap(sent, "blk", 1).astype(F32)
    total = part[0]
    arrived = [swap(part[s].astype(HALF), "blk", 2 * s) for s in range(1, pairs)]
    for value in arrived:
        total = total + value.astype(F32)
    return total


def grp_sum(slots):
    total = slots[0]
    arrived = [swap(slots[s].astype(HALF), "grp", s) for s in range(1, slots.shape[0])]
    for value in arrived:
        total = total + value.astype(F32)
    return total


def gather(value, axis, stride, count):
    return jnp.stack([value] + [swap(value, axis, stride * s) for s in range(1, count)])


def tree_sum(values):
    while len(values) > 1:
        values = [values[i] + values[i + 1] for i in range(0, len(values), 2)]
    return values[0]


def gather_all(piece, blk, grp):
    near = gather(gather(piece, "grp", 1, grp), "blk", 2, blk // 2)
    return near, swap(near, "blk", 1)


def shards(
    trial_vec,
    resid_vec,
    search_dir,
    trial_img,
    search_img,
    dens_exch,
    dens_direct,
    screen_mat,
    coulomb,
    valence_energy,
    conduct_energy,
    valence_index,
    conduct_index,
    ritz_coef,
):
    excitons = resid_vec.shape[1]
    blk = lax.axis_size("blk")
    grp = lax.axis_size("grp")
    own_blk = lax.axis_index("blk")
    own_grp = lax.axis_index("grp")
    place = jnp.stack([own_blk, own_grp]).astype(jnp.int32)
    piece = coulomb.shape[0] // (blk * grp)
    resid_half = resid_vec.astype(HALF)

    kept_d, sent_d = project(dens_direct, resid_half, place, blk, grp)
    kept_e, sent_e = project(dens_exch, resid_half, place, blk, grp)

    seen_piece = grp_sum(spread_sum(kept_d, sent_d)).astype(HALF)
    seen_slots = gather(seen_piece, "grp", 1, grp)
    seen = jnp.concatenate(
        [lax.dynamic_index_in_dim(seen_slots, z ^ own_grp, 0, False) for z in range(grp)], axis=1
    )
    screened = spread_sum(*screen(screen_mat, seen, place, blk)).astype(HALF)
    near_d, far_d = gather_all(screened, blk, grp)

    own_coulomb = lax.dynamic_slice_in_dim(coulomb, (own_blk * grp + own_grp) * piece, piece, 0)
    proj = grp_sum(spread_sum(kept_e, sent_e))
    weighted = (own_coulomb[None, :] * proj).astype(HALF)
    near_e, far_e = gather_all(weighted, blk, grp)
    exch_term = expand(dens_exch, near_e, far_e, place, blk, grp, False)

    valence_hot = (
        valence_index[:, None] == jnp.arange(valence_energy.shape[0], dtype=jnp.int32)[None, :]
    ).astype(F32)
    conduct_hot = (
        conduct_index[:, None] == jnp.arange(conduct_energy.shape[0], dtype=jnp.int32)[None, :]
    ).astype(F32)
    gap = jnp.sum(conduct_hot * conduct_energy[None, :], axis=1) - jnp.sum(
        valence_hot * valence_energy[None, :], axis=1
    )
    basis = jnp.concatenate([trial_vec, resid_vec, search_dir], axis=1)
    trial_coef = ritz_coef[:excitons]
    resid_coef = ritz_coef[excitons : 2 * excitons]
    search_coef = ritz_coef[2 * excitons :]
    next_search = exact_dot(resid_vec, resid_coef) + exact_dot(search_dir, search_coef)
    next_trial = exact_dot(trial_vec, trial_coef) + next_search
    search_part = exact_dot(search_img, search_coef)
    trial_part = exact_dot(trial_img, trial_coef)
    early = gap[:, None] * resid_vec + 2.0 * exch_term

    direct_term = expand(dens_direct, near_d, far_d, place, blk, grp, True)
    resid_img = early - direct_term
    images = jnp.concatenate([trial_img, resid_img, search_img], axis=1)
    gram = lax.dot_general(basis, images, ACROSS_ROWS, precision=lax.Precision.HIGHEST)
    gram = gram + swap(gram, "blk", 1)
    gram = tree_sum([gram] + [swap(gram, "blk", 2 * s) for s in range(1, blk // 2)])
    gram_matrix = tree_sum([gram] + [swap(gram, "grp", s) for s in range(1, grp)])
    next_search_img = exact_dot(resid_img, resid_coef) + search_part
    next_trial_img = trial_part + next_search_img
    return (next_trial, next_trial_img, next_search, next_search_img, gram_matrix)


def solution(mesh):
    rows = P(("blk", "grp"), None)
    return jax.shard_map(
        shards,
        mesh=mesh,
        in_specs=(rows,) * 7
        + (P("grp", "blk"), P(), P(), P(), P(("blk", "grp")), P(("blk", "grp")), P()),
        out_specs=(rows,) * 4 + (P(),),
        check_vma=False,
    )
```

```python
import jax
import jax.numpy as jnp
from jax import lax
from jax.experimental import pallas as pl
from jax.experimental.pallas import tpu as pltpu
from jax.sharding import PartitionSpec as P


F32 = jnp.float32
HALF = jnp.bfloat16
ACROSS_ROWS = (((0,), (0,)), ((), ()))
ACROSS_LANES = (((1,), (1,)), ((), ()))


def exact_dot(left, right):
    return jnp.dot(left, right, precision=lax.Precision.HIGHEST)


def swap(value, axis, offset):
    size = lax.axis_size(axis)
    return lax.ppermute(value, axis, [(i, i ^ offset) for i in range(size)])


def project(dens_direct, dens_exch, resid_half, place, blk, grp):
    pairs, total = dens_direct.shape
    excitons = resid_half.shape[1]
    block = total // blk
    piece = block // grp

    def body(place_ref, resid_ref, kept_d, sent_d, kept_e, sent_e, keep_ref, send_ref):
        resid = resid_ref[...]
        for term, (kept_ref, sent_ref) in enumerate(((kept_d, sent_d), (kept_e, sent_e))):
            kept = lax.dot_general(resid, kept_ref[...], ACROSS_ROWS, preferred_element_type=F32)
            sent = lax.dot_general(resid, sent_ref[...], ACROSS_ROWS, preferred_element_type=F32)
            for z in range(grp):
                lanes = slice(z * piece, (z + 1) * piece)
                slot = z ^ place_ref[1]
                keep_ref[0, slot, term] = kept[:, lanes]
                send_ref[0, slot, term] = sent[:, lanes].astype(HALF)

    out_spec = pl.BlockSpec((1, grp, 2, excitons, piece), lambda j, at: (j, 0, 0, 0, 0))
    kept_spec = pl.BlockSpec((pairs, block), lambda j, at: (0, (2 * j) ^ at[0]))
    sent_spec = pl.BlockSpec((pairs, block), lambda j, at: (0, (2 * j + 1) ^ at[0]))
    shape = (blk // 2, grp, 2, excitons, piece)
    return pl.pallas_call(
        body,
        grid_spec=pltpu.PrefetchScalarGridSpec(
            num_scalar_prefetch=1,
            grid=(blk // 2,),
            in_specs=[
                pl.BlockSpec((pairs, excitons), lambda j, at: (0, 0)),
                kept_spec,
                sent_spec,
                kept_spec,
                sent_spec,
            ],
            out_specs=[out_spec, out_spec],
        ),
        out_shape=[jax.ShapeDtypeStruct(shape, F32), jax.ShapeDtypeStruct(shape, HALF)],
        compiler_params=pltpu.CompilerParams(vmem_limit_bytes=16 * 2**20),
    )(place, resid_half, dens_direct, dens_direct, dens_exch, dens_exch)


def screen(screen_mat, seen, place, blk):
    rows, cols = screen_mat.shape
    excitons = seen.shape[0]
    piece = rows // blk
    splits = 2 if cols % 256 == 0 else 1
    width = cols // splits

    def body(place_ref, seen_ref, kept_ref, sent_ref, keep_ref, send_ref, acc_ref):
        kept = lax.dot_general(
            seen_ref[...], kept_ref[...], ACROSS_LANES, preferred_element_type=F32
        )
        sent = lax.dot_general(
            seen_ref[...], sent_ref[...], ACROSS_LANES, preferred_element_type=F32
        )
        step = pl.program_id(1)

        @pl.when(step == 0)
        def _():
            keep_ref[0] = kept
            acc_ref[...] = sent

        @pl.when(step > 0)
        def _():
            keep_ref[0] += kept
            acc_ref[...] += sent

        @pl.when(step == splits - 1)
        def _():
            send_ref[0] = acc_ref[...].astype(HALF)

    out_spec = pl.BlockSpec((1, excitons, piece), lambda j, k, at: (j, 0, 0))
    shape = (blk // 2, excitons, piece)
    return pl.pallas_call(
        body,
        grid_spec=pltpu.PrefetchScalarGridSpec(
            num_scalar_prefetch=1,
            grid=(blk // 2, splits),
            in_specs=[
                pl.BlockSpec((excitons, width), lambda j, k, at: (0, k)),
                pl.BlockSpec((piece, width), lambda j, k, at: ((2 * j) ^ at[0], k)),
                pl.BlockSpec((piece, width), lambda j, k, at: ((2 * j + 1) ^ at[0], k)),
            ],
            out_specs=[out_spec, out_spec],
            scratch_shapes=[pltpu.VMEM((excitons, piece), F32)],
        ),
        out_shape=[jax.ShapeDtypeStruct(shape, F32), jax.ShapeDtypeStruct(shape, HALF)],
        compiler_params=pltpu.CompilerParams(vmem_limit_bytes=24 * 2**20),
    )(place, seen, screen_mat, screen_mat)


def expand(dens_direct, dens_exch, near, far, place, blk, grp):
    pairs = dens_direct.shape[0]
    excitons, piece = near.shape[3:]

    def body(place_ref, direct_ref, exch_ref, near_ref, far_ref, out_ref):
        direct = jnp.zeros((pairs, excitons), F32)
        exch = jnp.zeros((pairs, excitons), F32)
        odd = place_ref[0] & 1
        for pair in range(blk // 2):
            slot = pair ^ (place_ref[0] >> 1)
            for z in range(grp):
                deep = z ^ place_ref[1]
                near_d, far_d = near_ref[slot, deep, 0], far_ref[slot, deep, 0]
                near_e, far_e = near_ref[slot, deep, 1], far_ref[slot, deep, 1]
                for bit in range(2):
                    b = 2 * pair + bit
                    at = (z * blk + b) * piece
                    direct += lax.dot_general(
                        direct_ref[:, at : at + piece],
                        jnp.where(odd == bit, near_d, far_d),
                        ACROSS_LANES,
                        preferred_element_type=F32,
                    )
                    at = (b * grp + z) * piece
                    exch += lax.dot_general(
                        exch_ref[:, at : at + piece],
                        jnp.where(odd == bit, near_e, far_e),
                        ACROSS_LANES,
                        preferred_element_type=F32,
                    )
        out_ref[...] = 2.0 * exch - direct

    vmem = pl.BlockSpec(memory_space=pltpu.VMEM)
    return pl.pallas_call(
        body,
        in_specs=[pl.BlockSpec(memory_space=pltpu.SMEM), vmem, vmem, vmem, vmem],
        out_specs=vmem,
        out_shape=jax.ShapeDtypeStruct((pairs, excitons), F32),
        compiler_params=pltpu.CompilerParams(vmem_limit_bytes=24 * 2**20),
    )(place, dens_direct, dens_exch, near, far)


def spread_sum(kept, sent):
    pairs = kept.shape[0]
    part = kept + swap(sent, "blk", 1).astype(F32)
    total = part[0]
    arrived = [swap(part[s].astype(HALF), "blk", 2 * s) for s in range(1, pairs)]
    for value in arrived:
        total = total + value.astype(F32)
    return total


def halve(slots, axis, stride):
    count = slots.shape[0]
    while count > 1:
        count //= 2
        sent = swap(slots[count:].astype(HALF), axis, stride * count)
        slots = slots[:count] + sent.astype(F32)
    return slots[0]


def gather(value, axis, stride, count):
    return jnp.stack([value] + [swap(value, axis, stride * s) for s in range(1, count)])


def double(value, axis, stride, count):
    slots = value[None]
    while slots.shape[0] < count:
        slots = jnp.concatenate([slots, swap(slots, axis, stride * slots.shape[0])])
    return slots


def gather_all(piece, blk, grp):
    near = gather(double(piece, "grp", 1, grp), "blk", 2, blk // 2)
    return near, swap(near, "blk", 1)


def total_of(value, axis):
    offset = 1
    while offset < lax.axis_size(axis):
        value = value + swap(value, axis, offset)
        offset *= 2
    return value


def shards(
    trial_vec,
    resid_vec,
    search_dir,
    trial_img,
    search_img,
    dens_exch,
    dens_direct,
    screen_mat,
    coulomb,
    valence_energy,
    conduct_energy,
    valence_index,
    conduct_index,
    ritz_coef,
):
    excitons = resid_vec.shape[1]
    blk = lax.axis_size("blk")
    grp = lax.axis_size("grp")
    own_blk = lax.axis_index("blk")
    own_grp = lax.axis_index("grp")
    place = jnp.stack([own_blk, own_grp]).astype(jnp.int32)
    piece = coulomb.shape[0] // (blk * grp)
    resid_half = resid_vec.astype(HALF)

    projected = halve(
        spread_sum(*project(dens_direct, dens_exch, resid_half, place, blk, grp)), "grp", 1
    )
    seen_slots = double(projected[0].astype(HALF), "grp", 1, grp)
    seen = jnp.concatenate(
        [lax.dynamic_index_in_dim(seen_slots, z ^ own_grp, 0, False) for z in range(grp)], axis=1
    )
    own_coulomb = lax.dynamic_slice_in_dim(coulomb, (own_blk * grp + own_grp) * piece, piece, 0)
    weighted = (own_coulomb[None, :] * projected[1]).astype(HALF)

    kept_s, sent_s = screen(screen_mat, seen, place, blk)
    screened = halve(kept_s + swap(sent_s, "blk", 1).astype(F32), "blk", 2).astype(HALF)
    near, far = gather_all(jnp.stack([screened, weighted]), blk, grp)

    valence_hot = (
        valence_index[:, None] == jnp.arange(valence_energy.shape[0], dtype=jnp.int32)[None, :]
    ).astype(F32)
    conduct_hot = (
        conduct_index[:, None] == jnp.arange(conduct_energy.shape[0], dtype=jnp.int32)[None, :]
    ).astype(F32)
    gap = jnp.sum(conduct_hot * conduct_energy[None, :], axis=1) - jnp.sum(
        valence_hot * valence_energy[None, :], axis=1
    )
    basis = jnp.concatenate([trial_vec, resid_vec, search_dir], axis=1)
    trial_coef = ritz_coef[:excitons]
    resid_coef = ritz_coef[excitons : 2 * excitons]
    search_coef = ritz_coef[2 * excitons :]
    next_search = exact_dot(resid_vec, resid_coef) + exact_dot(search_dir, search_coef)
    next_trial = exact_dot(trial_vec, trial_coef) + next_search
    search_part = exact_dot(search_img, search_coef)
    trial_part = exact_dot(trial_img, trial_coef)
    early = gap[:, None] * resid_vec

    resid_img = early + expand(dens_direct, dens_exch, near, far, place, blk, grp)
    images = jnp.concatenate([trial_img, resid_img, search_img], axis=1)
    gram = lax.dot_general(basis, images, ACROSS_ROWS, precision=lax.Precision.HIGHEST)
    gram_matrix = total_of(total_of(gram, "blk"), "grp")
    next_search_img = exact_dot(resid_img, resid_coef) + search_part
    next_trial_img = trial_part + next_search_img
    return (next_trial, next_trial_img, next_search, next_search_img, gram_matrix)


def solution(mesh):
    rows = P(("blk", "grp"), None)
    return jax.shard_map(
        shards,
        mesh=mesh,
        in_specs=(rows,) * 7
        + (P("grp", "blk"), P(), P(), P(), P(("blk", "grp")), P(("blk", "grp")), P()),
        out_specs=(rows,) * 4 + (P(),),
        check_vma=False,
    )
```
